512 devices in a mesh: blk: 8 (over z), grid: 64 (over y, x, core).
Axes of the slice: x: 4, y: 8, z: 8, core: 2. Of those that a mesh axis runs over, the one named last changes fastest.
Arguments:
- centers: bfloat16 [65536, 512], P(('blk', 'grid')), as said below
- weights: float32 [65536, 1000], P(('blk', 'grid')), may hold values from -4 to 4
- batch_index: int32 [512], replicated, may hold values from 0 to 65535, as said below
- labels: int32 [512], replicated, may hold values from 0 to 999
- sub_index: int32 [4096], P(('blk', 'grid')), may hold values from 0 to 127
- eigvecs: bfloat16 [4096, 160], P(('blk', 'grid')), may hold values from -0.09375 to 0.09375
- scales: float32 [160], replicated, may hold values from 1 to 16
Outputs:
- predictions: bfloat16 [512, 1000], replicated
- center_grad: bfloat16 [65536, 1000], P(('blk', 'grid'))
- sub_increment: float32 [4096, 1000], P(('blk', 'grid'))
The draws below stay inside these ranges and needn't reach their ends.
Inputs may be any that keep to these rules, and one draw needn't show every extreme that they name: Each device's block of 128 centers is named by exactly 512 / 512 entries of batch_index. sub_index: entry i names center (i // 8) * 128 + sub_index[i]. centers: row scales of order one.
All inputs are finite; a program needn't handle non-finite values.
Results may differ from the reference program's by a relative error of at most 0.0011.
The reference program's roundings to bfloat16 on the way (of `batch`, `kbz`, `resid`, `subset`, `ksb` and `kzs`) count: a program that leaves them out, or rounds other values in their place, can miss the bound.
Values may be sent and summed in bfloat16 or wider, within the bound.
No kernel may reach another device: no remote copies, remote signals or barrier semaphores. Data moves between devices by JAX's collectives and lax.ppermute only.
A program may use at most 64 MiB of HBM per device.

```python
import math
import jax
import jax.numpy as jnp
from jax import lax

D = 512
C = 1000
RANK = 160
B = 512
CENTER_DEV = 128
SUB_DEV = 8
GROUPS = 512
CENTERS = 65536
SUBSET = 4096
N_BLK = 8
N_GRID = 64


def draw_centers(key, part):
    first = jax.random.fold_in(key, 11)
    second = jax.random.fold_in(key, 12)
    row_scale = jnp.exp(jax.random.uniform(first, (CENTERS, 1), jnp.float32, jnp.log(0.25), 0.0))
    values = jax.random.normal(second, (CENTERS, D), jnp.float32)
    return (row_scale * values).astype(jnp.bfloat16)


def draw_batch_index(key, part):
    first = jax.random.fold_in(key, 21)
    second = jax.random.fold_in(key, 22)
    share = B // GROUPS
    owners = jnp.repeat(jnp.arange(GROUPS, dtype=jnp.int32), share, total_repeat_length=B)
    owners = jax.random.permutation(first, owners)
    within = jax.random.randint(second, (B,), 0, CENTER_DEV, jnp.int32)
    return (owners * CENTER_DEV + within).astype(jnp.int32)


def with_ends(array, stream_key, least, largest):
    place = [jax.random.randint(jax.random.fold_in(stream_key, axis), (), 0, length) for axis, length in enumerate(array.shape)]
    main_axis = array.shape.index(max(array.shape))
    next_to = place[:main_axis] + [(place[main_axis] + 1) % array.shape[main_axis]] + place[main_axis + 1:]
    return array.at[tuple(place)].set(least).at[tuple(next_to)].set(largest)


def block_scale(own_key, dims, split, low, largest):
    gain = 1.0
    for dim, shards_of in split:
        steps = jax.random.uniform(jax.random.fold_in(jax.random.fold_in(own_key, 6), dim), (shards_of,), jnp.float32, low / len(split), largest / len(split))
        gain = gain * jnp.repeat(jnp.exp(steps), dims[dim] // shards_of).reshape((-1,) + (1,) * (len(dims) - 1 - dim))
    return gain


def noise(own_key, dims, scale, reach, cuts=(), held_as=jnp.bfloat16):
    level = block_scale(own_key, dims, cuts, -0.22, 0.18) if cuts else 1.0
    array = jax.random.normal(own_key, dims, jnp.float32) * scale * level
    return jnp.minimum(jnp.maximum(array, -reach), reach).astype(held_as)


def setup_inputs(seed: int = 0) -> dict:
    key_of = jax.random.split(jax.random.key(seed), 8)
    centers = draw_centers(jax.random.fold_in(key_of[7], 71), 0)
    weights = noise(key_of[1], (CENTERS, C), (D * (CENTER_DEV * N_BLK * N_GRID) ** -0.5 / 8), 4.0, ((0, 512),), jnp.float32)
    batch_index = draw_batch_index(jax.random.fold_in(key_of[7], 71), 0)
    labels = with_ends(jax.random.randint(key_of[3], (B,), 0, C), jax.random.fold_in(key_of[3], 1), 0, C - 1).astype(jnp.int32)
    sub_index = with_ends(jax.random.randint(key_of[4], (SUBSET,), 0, CENTER_DEV), jax.random.fold_in(key_of[4], 1), 0, CENTER_DEV - 1).astype(jnp.int32)
    eigvecs = noise(key_of[5], (SUBSET, RANK), SUBSET ** -0.5, 0.09375, ((0, 512),))
    scales = jnp.clip(jnp.exp(jax.random.uniform(key_of[6], (RANK,), jnp.float32, math.log(1.0), math.log(16.0))), 1.0, 16.0)
    return {"centers": centers, "weights": weights, "batch_index": batch_index, "labels": labels, "sub_index": sub_index, "eigvecs": eigvecs, "scales": scales}


SOFTEN = 1.0
SPREAD = 4.0

def kernel(left, right):
    left_sq = lax.optimization_barrier(jnp.sum(jnp.square(left.astype(jnp.float32)), axis=1))
    right_sq = lax.optimization_barrier(jnp.sum(jnp.square(right.astype(jnp.float32)), axis=1))
    cross = lax.dot_general(left, right, (((1,), (1,)), ((), ())), preferred_element_type=jnp.float32)
    dist = jnp.sqrt(jnp.maximum(left_sq[:, None] + right_sq[None, :] - 2.0 * cross, 0.0) + SOFTEN)
    return jnp.exp(-dist / SPREAD)

def reference(centers, weights, batch_index, labels, sub_index, eigvecs, scales):
    groups = N_BLK * N_GRID
    batch = jnp.take(centers, batch_index, axis=0)
    blocks_z = centers.reshape(groups, CENTER_DEV, D)
    blocks_w = weights.reshape(groups, CENTER_DEV, C)

    def accumulate(carry, item):
        zrows, wrows = item
        kbz = kernel(batch, zrows).astype(jnp.bfloat16)
        return (carry + jnp.dot(kbz, wrows.astype(jnp.bfloat16), preferred_element_type=jnp.float32), None)
    total, unused = lax.scan(accumulate, jnp.zeros((B, C), jnp.float32), (blocks_z, blocks_w))
    predictions = total.astype(jnp.bfloat16)
    onehot = (labels[:, None] == jnp.arange(C, dtype=jnp.int32)[None, :]).astype(jnp.float32)
    resid = (total - onehot).astype(jnp.bfloat16)
    rows = (jnp.arange(SUBSET, dtype=jnp.int32) // SUB_DEV * CENTER_DEV + sub_index).astype(jnp.int32)
    subset = jnp.take(centers, rows, axis=0)
    ksb = kernel(subset, batch).astype(jnp.bfloat16)
    inner = jnp.dot(ksb, resid, preferred_element_type=jnp.float32)
    coeff = jnp.dot(eigvecs.astype(jnp.float32).T, inner, precision=lax.Precision.HIGHEST)
    scaled = scales[:, None] * coeff
    sub_increment = jnp.dot(eigvecs.astype(jnp.float32), scaled, precision=lax.Precision.HIGHEST)

    def gradient(zrows):
        kbz = kernel(batch, zrows).astype(jnp.bfloat16)
        first = lax.dot_general(kbz, resid, (((0,), (0,)), ((), ())), preferred_element_type=jnp.float32)
        kzs = kernel(zrows, subset).astype(jnp.bfloat16)
        kze = jnp.dot(kzs, eigvecs, preferred_element_type=jnp.float32)
        correction = jnp.dot(kze, scaled, precision=lax.Precision.HIGHEST)
        return (first - correction).astype(jnp.bfloat16)
    center_grad = lax.map(gradient, blocks_z).reshape(CENTERS, C)
    return (predictions, center_grad, sub_increment)
```

```python
import jax
import jax.numpy as jnp
from jax import lax
from jax.sharding import Mesh
from jax.sharding import PartitionSpec as P

Z, Y, X, CORE = "blk", "grid_0", "grid_1", "grid_2"
ALL = (Z, Y, X, CORE)
PLANE = (Z, Y)

SOFTEN = 1.0
SPREAD = 4.0
LARGEST = 3.0e38
TILE = 128


def up_to(size, step):
    return -(-size // step) * step


def exchange(pieces, axis):
    return lax.all_to_all(pieces, axis, 0, 0, tiled=True)


def to_each(array, axis):
    return jnp.broadcast_to(array[None], (lax.axis_size(axis), *array.shape))


def from_other_core(array):
    return lax.ppermute(array, CORE, [(0, 1), (1, 0)])


def squares(rows):
    return jnp.sum(jnp.square(rows.astype(jnp.float32)), axis=1)


def kernel(left, right):
    cross = lax.dot_general(
        left, right, (((1,), (1,)), ((), ())), preferred_element_type=jnp.float32
    )
    apart = squares(left)[:, None] + squares(right)[None, :] - 2.0 * cross
    soft = jnp.minimum(jnp.maximum(apart, 0.0) + SOFTEN, LARGEST)
    return jnp.exp(soft * lax.rsqrt(soft) * (-1.0 / SPREAD)).astype(jnp.bfloat16)


def rounded(array):
    return lax.reduce_precision(array, exponent_bits=8, mantissa_bits=7)


def parts_of(array, count):
    parts = []
    for _ in range(count):
        part = rounded(array)
        parts.append(part.astype(jnp.bfloat16))
        array = array - part
    return parts


def dot(left, right, contract=((1,), (0,))):
    return lax.dot_general(left, right, (contract, ((), ())), preferred_element_type=jnp.float32)


def with_columns(array, columns):
    return jnp.pad(array, [(0, 0)] * (array.ndim - 1) + [(0, columns - array.shape[-1])])


def local(centers, weights, batch_index, labels, sub_index, eigvecs, scales):
    nx, nplane = lax.axis_size(X), lax.axis_size(PLANE)
    held, depth = centers.shape
    classes = weights.shape[1]
    points, rank = eigvecs.shape
    me = lax.axis_index(ALL)
    my_x = lax.axis_index(X)
    my_core = lax.axis_index(CORE)
    block = up_to(-(-classes // nx), TILE)
    ranks = rank // nx
    wide = up_to(block + 2 * ranks + 1, TILE)
    lines = depth // 32

    owner = batch_index // held
    within = batch_index % held
    row = jnp.sum(jnp.where(owner == me, within, 0))
    mine = lax.dynamic_slice(centers, (row, 0), (1, depth))
    picks = sub_index[:, None] == jnp.arange(held, dtype=jnp.int32)[None, :]
    picks = picks.astype(jnp.bfloat16)
    subset = dot(picks, centers).astype(jnp.bfloat16)
    spread_vecs = dot(picks, eigvecs, ((0,), (0,)))

    def by_x(array):
        return jnp.moveaxis(array.reshape(array.shape[0], nx, -1), 1, 0)

    high, low = parts_of(spread_vecs, 2)
    wts = by_x(with_columns(weights.astype(jnp.bfloat16), nx * block))
    room = wide - block - 2 * ranks - 32
    side = jnp.pad(mine.reshape(lines, 32), ((0, held - lines), (room, 0)))
    own_columns = jnp.concatenate([wts, by_x(high), by_x(low), to_each(side, X)], axis=2)
    along_x = exchange(jnp.concatenate([to_each(centers, X), own_columns], axis=2), X)
    opposite = from_other_core(along_x)

    near_rows = along_x[:, :lines, depth + wide - 32 :].reshape(nx, depth)
    half = depth * nx // points
    near_rows = jnp.concatenate(jnp.split(near_rows, points // nx, axis=1), axis=0)
    vec_at = depth + half
    packed = jnp.concatenate([subset, near_rows, eigvecs], axis=1)
    in_plane = exchange(to_each(packed, PLANE), PLANE)
    batch = in_plane[:, :, depth:vec_at].reshape(nplane, points // nx, nx, half)
    batch = jnp.concatenate([batch[:, i] for i in range(points // nx)], axis=2)
    batch = batch.reshape(nplane * nx, depth)
    sub_rows = in_plane[:, :, :depth].reshape(nplane * points, depth)
    vec_rows = in_plane[:, :, vec_at:].reshape(nplane * points, rank)

    here = along_x[:, :, :depth].reshape(nx * held, depth)
    there = opposite[:, :, :depth].reshape(nx * held, depth)
    sums = dot(kernel(batch, here), along_x[:, :, depth:].reshape(nx * held, wide))
    sums = sums + dot(kernel(batch, there), opposite[:, :, depth:].reshape(nx * held, wide))
    arrived = exchange(sums.reshape(nplane, nx, wide), PLANE)

    other_batch = from_other_core(batch)
    kze = dot(kernel(here, sub_rows), vec_rows)
    kze = kze + from_other_core(dot(kernel(there, sub_rows), vec_rows))
    kbz = kernel(centers, batch)
    other_kbz = kernel(centers, other_batch)

    total = jnp.sum(arrived, axis=0)
    first_row = (lax.axis_index(PLANE) * nx + jnp.arange(nx, dtype=jnp.int32)) * 2 + my_core
    row_labels = jnp.sum(jnp.where(owner[None, :] == first_row[:, None], labels[None, :], 0), axis=1)
    mark = row_labels[:, None] == my_x * block + jnp.arange(block, dtype=jnp.int32)[None, :]
    at_label = jnp.sum(jnp.where(mark, total[:, :block] - 1.0, 0.0), axis=1, keepdims=True)
    proj = total[:, block : block + ranks] + total[:, block + ranks : block + 2 * ranks]
    proj_high, proj_low = parts_of(proj, 2)
    ready = jnp.concatenate(
        [total[:, :block].astype(jnp.bfloat16), proj_high, proj_low, at_label.astype(jnp.bfloat16)],
        axis=1,
    )
    rows = exchange(to_each(with_columns(ready, wide), PLANE), PLANE).reshape(-1, wide)

    kze_parts = with_columns(jnp.concatenate(parts_of(kze, 2), axis=1), wide)
    last = jnp.concatenate([to_each(rows, X), kze_parts.reshape(nx, held, wide)], axis=1)
    last = exchange(last, X)
    own_half = last[:, : nplane * nx]
    other_half = from_other_core(own_half)
    kze_sum = jnp.sum(last[:, nplane * nx :].astype(jnp.float32), axis=0)
    kze_sum = kze_sum[:, :rank] + kze_sum[:, rank : 2 * rank]
    left = jnp.concatenate([kze_sum, -eigvecs.astype(jnp.float32)], axis=0) * scales[None, :]

    numbers = jnp.arange(nplane * nx, dtype=jnp.int32)
    gradient, predictions = 0.0, 0.0
    for half_rows, core, near in ((own_half, my_core, kbz), (other_half, 1 - my_core, other_kbz)):
        devices = numbers * 2 + core
        chosen = owner[:, None] == devices[None, :]
        label = jnp.sum(jnp.where(chosen, labels[:, None], 0), axis=0)
        pred = jnp.concatenate([half_rows[i, :, :block] for i in range(nx)], axis=1)[:, :classes]
        predictions = predictions + dot(chosen.astype(jnp.bfloat16), pred)
        at = half_rows[:, :, block + 2 * ranks]
        column = jnp.arange(classes, dtype=jnp.int32)[None, :]
        mark = label[:, None] == column
        value = jnp.sum(
            jnp.where((label // block)[None, :] == jnp.arange(nx)[:, None], at.astype(jnp.float32), 0.0),
            axis=0,
        )
        resid = jnp.where(mark, value[:, None].astype(jnp.bfloat16), pred)
        proj = half_rows[:, :, block : block + ranks].astype(jnp.float32)
        proj = proj + half_rows[:, :, block + ranks : block + 2 * ranks].astype(jnp.float32)
        proj = jnp.moveaxis(proj, 0, 1).reshape(nplane * nx, rank)
        back = lax.dot_general(
            left, proj, (((1,), (1,)), ((), ())), precision=lax.Precision.HIGHEST
        )
        near = jnp.pad(near.astype(jnp.float32), ((0, points), (0, 0)))
        pieces = parts_of(near - back, 3)
        gradient = gradient + sum(dot(piece, resid) for piece in pieces)
    center_grad = gradient[:held].astype(jnp.bfloat16)
    return (predictions.astype(jnp.bfloat16), center_grad, gradient[held:])


def solution(mesh):
    finer = Mesh(mesh.devices.reshape(mesh.shape["blk"], 8, 4, 2), ALL)
    return jax.shard_map(
        local,
        mesh=finer,
        in_specs=(
            P(ALL, None),
            P(ALL, None),
            P(),
            P(),
            P(ALL),
            P(ALL, None),
            P(),
        ),
        out_specs=(P(), P(ALL, None), P(ALL, None)),
        check_vma=False,
    )
```

```python
import jax
import jax.numpy as jnp
from jax import lax
from jax.sharding import Mesh
from jax.sharding import PartitionSpec as P

Z, Y, X, CORE = "blk", "grid_0", "grid_1", "grid_2"
ALL = (Z, Y, X, CORE)
PLANE = (Z, Y)

SOFTEN = 1.0
SPREAD = 4.0
LARGEST = 3.0e38
TILE = 128


def up_to(size, step):
    return -(-size // step) * step


def exchange(pieces, axis):
    return lax.all_to_all(pieces, axis, 0, 0, tiled=True)


def to_each(array, axis):
    return jnp.broadcast_to(array[None], (lax.axis_size(axis), *array.shape))


def from_other_core(array):
    return lax.ppermute(array, CORE, [(0, 1), (1, 0)])


def to_next(array, axis, step):
    count = lax.axis_size(axis)
    return lax.ppermute(array, axis, [(i, (i + step) % count) for i in range(count)])


def squares(rows):
    return jnp.sum(jnp.square(rows.astype(jnp.float32)), axis=1)


def kernel(left, right):
    cross = lax.dot_general(
        left, right, (((1,), (1,)), ((), ())), preferred_element_type=jnp.float32
    )
    apart = squares(left)[:, None] + squares(right)[None, :] - 2.0 * cross
    soft = jnp.minimum(jnp.maximum(apart, 0.0) + SOFTEN, LARGEST)
    return jnp.exp(soft * lax.rsqrt(soft) * (-1.0 / SPREAD)).astype(jnp.bfloat16)


def rounded(array):
    return lax.reduce_precision(array, exponent_bits=8, mantissa_bits=7)


def parts_of(array, count):
    parts = []
    for _ in range(count):
        part = rounded(array)
        parts.append(part.astype(jnp.bfloat16))
        array = array - part
    return parts


def dot(left, right, contract=((1,), (0,))):
    return lax.dot_general(left, right, (contract, ((), ())), preferred_element_type=jnp.float32)


def with_columns(array, columns):
    return jnp.pad(array, [(0, 0)] * (array.ndim - 1) + [(0, columns - array.shape[-1])])


def step(centers, weights, batch_index, labels, sub_index, eigvecs, scales):
    nx, nplane = lax.axis_size(X), lax.axis_size(PLANE)
    held, depth = centers.shape
    classes = weights.shape[1]
    points, rank = eigvecs.shape
    me = lax.axis_index(ALL)
    my_x = lax.axis_index(X)
    my_core = lax.axis_index(CORE)
    block = up_to(-(-classes // nx), TILE)
    ranks = rank // nx
    wide = up_to(block + 2 * ranks + 1, TILE)
    half = nplane * nx
    label_at = 2 * ranks

    owner = batch_index // held
    within = batch_index % held
    row = jnp.sum(jnp.where(owner == me, within, 0))
    mine = lax.dynamic_slice(centers, (row, 0), (1, depth))
    picks = sub_index[:, None] == jnp.arange(held, dtype=jnp.int32)[None, :]
    picks = picks.astype(jnp.bfloat16)
    subset = dot(picks, centers).astype(jnp.bfloat16)
    packed = jnp.concatenate([subset, eigvecs, mine.reshape(points, -1)], axis=1)
    in_plane = exchange(to_each(packed, PLANE), PLANE)
    sub_rows = in_plane[:, :, :depth].reshape(nplane * points, depth)
    vec_rows = in_plane[:, :, depth : depth + rank].reshape(nplane * points, rank)
    column = in_plane[:, :, depth + rank :].reshape(nplane, depth)
    batch = exchange(to_each(column, X), X).reshape(half, depth)

    def by_x(array):
        return jnp.moveaxis(array.reshape(array.shape[0], nx, -1), 1, 0)

    high, low = parts_of(dot(picks, eigvecs, ((0,), (0,))), 2)
    wts = by_x(with_columns(weights.astype(jnp.bfloat16), nx * block))
    shares = with_columns(jnp.concatenate([wts, by_x(high), by_x(low)], axis=2), wide)

    def share_for(x):
        share = lax.dynamic_index_in_dim(shares, x % nx, 0, keepdims=False)
        return jnp.concatenate([centers, share], axis=1)

    around = [share_for(my_x)] + [to_next(share_for(my_x + k), X, k) for k in range(1, nx)]
    around = jnp.concatenate(around, axis=0)
    opposite = from_other_core(around)
    here, there = around[:, :depth], opposite[:, :depth]

    sums = dot(kernel(batch, here), around[:, depth:])
    sums = sums + dot(kernel(batch, there), opposite[:, depth:])
    arrived = exchange(sums.reshape(nplane, nx, wide), PLANE)

    other_batch = from_other_core(batch)
    kze = dot(kernel(here, sub_rows), vec_rows)
    kze = kze + from_other_core(dot(kernel(there, sub_rows), vec_rows))
    kze_sum = kze[:held]
    for k in range(1, nx):
        kze_sum = kze_sum + to_next(kze[k * held : (k + 1) * held], X, -k)
    kbz = kernel(centers, batch)
    other_kbz = kernel(centers, other_batch)

    def device_of(number, core):
        return (number % nplane * nx + number // nplane) * 2 + core

    total = jnp.sum(arrived, axis=0)
    numbers = lax.axis_index(PLANE) * nx + jnp.arange(nx, dtype=jnp.int32)
    found = owner[None, :] == device_of(numbers, my_core)[:, None]
    row_labels = jnp.sum(jnp.where(found, labels[None, :], 0), axis=1)
    mark = row_labels[:, None] == my_x * block + jnp.arange(block, dtype=jnp.int32)[None, :]
    at_label = jnp.sum(jnp.where(mark, total[:, :block] - 1.0, 0.0), axis=1, keepdims=True)
    proj = total[:, block : block + ranks] + total[:, block + ranks : block + 2 * ranks]
    ready = [total[:, :block].astype(jnp.bfloat16), *parts_of(proj, 2), at_label.astype(jnp.bfloat16)]
    ready = with_columns(jnp.concatenate(ready, axis=1), wide)
    rows = exchange(to_each(ready, PLANE), PLANE).reshape(half, wide)
    own_half = exchange(to_each(rows, X), X)
    other_half = from_other_core(own_half)

    left = jnp.concatenate([kze_sum, -eigvecs.astype(jnp.float32)], axis=0) * scales[None, :]
    left = left.reshape(held + points, nx, ranks)
    left = with_columns(jnp.concatenate([left, left], axis=2), wide - block)
    left = parts_of(left.reshape(held + points, nx * (wide - block)), 2)

    numbers = jnp.arange(half, dtype=jnp.int32)
    gradient, predictions = 0.0, 0.0
    for half_rows, core, near in ((own_half, my_core, kbz), (other_half, 1 - my_core, other_kbz)):
        chosen = owner[:, None] == device_of(numbers, core)[None, :]
        label = jnp.sum(jnp.where(chosen, labels[:, None], 0), axis=0)
        pred = jnp.concatenate([half_rows[i, :, :block] for i in range(nx)], axis=1)[:, :classes]
        predictions = predictions + dot(chosen.astype(jnp.bfloat16), pred)
        value = half_rows[:, :, block + label_at].astype(jnp.float32).sum(axis=0)
        mark = label[:, None] == jnp.arange(classes, dtype=jnp.int32)[None, :]
        resid = jnp.where(mark, value[:, None].astype(jnp.bfloat16), pred)
        proj = jnp.concatenate([half_rows[i, :, block:] for i in range(nx)], axis=1)
        back = sum(dot(piece, proj, ((1,), (1,))) for piece in left)
        near = jnp.pad(near.astype(jnp.float32), ((0, points), (0, 0)))
        gradient = gradient + sum(dot(piece, resid) for piece in parts_of(near - back, 2))
    center_grad = gradient[:held].astype(jnp.bfloat16)
    return (predictions.astype(jnp.bfloat16), center_grad, gradient[held:])


def solution(mesh):
    finer = Mesh(mesh.devices.reshape(mesh.shape["blk"], 8, 4, 2), ALL)
    return jax.shard_map(
        step,
        mesh=finer,
        in_specs=(
            P(ALL, None),
            P(ALL, None),
            P(),
            P(),
            P(ALL),
            P(ALL, None),
            P(),
        ),
        out_specs=(P(), P(ALL, None), P(ALL, None)),
        check_vma=False,
    )
```

```python
import jax
import jax.numpy as jnp
from jax import lax
from jax.sharding import Mesh
from jax.sharding import PartitionSpec as P

Z, Y, X, CORE = "blk", "grid_0", "grid_1", "grid_2"
ALL = (Z, Y, X, CORE)
PLANE = (Z, Y)

SOFTEN = 1.0
SPREAD = 4.0
LARGEST = 3.0e38
TILE = 128


def up_to(size, step):
    return -(-size // step) * step


def exchange(pieces, axis):
    return lax.all_to_all(pieces, axis, 0, 0, tiled=True)


def to_each(array, axis):
    return jnp.broadcast_to(array[None], (lax.axis_size(axis), *array.shape))


def from_other_core(array):
    return lax.ppermute(array, CORE, [(0, 1), (1, 0)])


def to_next(array, axis, step):
    count = lax.axis_size(axis)
    return lax.ppermute(array, axis, [(i, (i + step) % count) for i in range(count)])


def squares(rows):
    return jnp.sum(jnp.square(rows.astype(jnp.float32)), axis=1)


def kernel(left, right):
    cross = lax.dot_general(
        left, right, (((1,), (1,)), ((), ())), preferred_element_type=jnp.float32
    )
    apart = squares(left)[:, None] + squares(right)[None, :] - 2.0 * cross
    soft = jnp.minimum(jnp.maximum(apart, 0.0) + SOFTEN, LARGEST)
    return jnp.exp(soft * lax.rsqrt(soft) * (-1.0 / SPREAD)).astype(jnp.bfloat16)


def rounded(array):
    return lax.reduce_precision(array, exponent_bits=8, mantissa_bits=7)


def parts_of(array, count):
    parts = []
    for _ in range(count):
        part = rounded(array)
        parts.append(part.astype(jnp.bfloat16))
        array = array - part
    return parts


def dot(left, right, contract=((1,), (0,))):
    return lax.dot_general(left, right, (contract, ((), ())), preferred_element_type=jnp.float32)


def with_columns(array, columns):
    return jnp.pad(array, [(0, 0)] * (array.ndim - 1) + [(0, columns - array.shape[-1])])


def step(centers, weights, batch_index, labels, sub_index, eigvecs, scales):
    nx, nplane = lax.axis_size(X), lax.axis_size(PLANE)
    held, depth = centers.shape
    classes = weights.shape[1]
    points, rank = eigvecs.shape
    me = lax.axis_index(ALL)
    my_x = lax.axis_index(X)
    my_core = lax.axis_index(CORE)
    block = up_to(-(-classes // nx), TILE)
    ranks = rank // nx
    wide = up_to(block + 2 * ranks + 1, TILE)
    half = nplane * nx
    label_at = 2 * ranks

    owner = batch_index // held
    places = jnp.arange(held, dtype=jnp.int32)
    taken = jnp.any(batch_index[None, :] == (me * held + places)[:, None], axis=1)
    picks = sub_index[:, None] == places[None, :]
    chosen = jnp.concatenate([picks, taken[None, :]], axis=0).astype(jnp.bfloat16)
    picks = picks.astype(jnp.bfloat16)
    rows = dot(chosen, centers).astype(jnp.bfloat16)
    subset, mine = rows[:points], rows[points:]
    packed = jnp.concatenate([subset, eigvecs, mine.reshape(points, -1)], axis=1)
    in_plane = exchange(to_each(packed, PLANE), PLANE)
    sub_rows = in_plane[:, :, :depth].reshape(nplane * points, depth)
    vec_rows = in_plane[:, :, depth : depth + rank].reshape(nplane * points, rank)
    column = in_plane[:, :, depth + rank :].reshape(nplane, depth)
    batch = exchange(to_each(column, X), X).reshape(half, depth)

    def by_x(array):
        return jnp.moveaxis(array.reshape(array.shape[0], nx, -1), 1, 0)

    high, low = parts_of(dot(picks, eigvecs, ((0,), (0,))), 2)
    wts = by_x(with_columns(weights.astype(jnp.bfloat16), nx * block))
    shares = with_columns(jnp.concatenate([wts, by_x(high), by_x(low)], axis=2), wide)

    def share_for(x):
        share = lax.dynamic_index_in_dim(shares, x % nx, 0, keepdims=False)
        return jnp.concatenate([centers, share], axis=1)

    around = [share_for(my_x)] + [to_next(share_for(my_x + k), X, k) for k in range(1, nx)]
    around = jnp.concatenate(around, axis=0)
    opposite = from_other_core(around)
    here, there = around[:, :depth], opposite[:, :depth]

    sums = dot(kernel(batch, here), around[:, depth:])
    sums = sums + dot(kernel(batch, there), opposite[:, depth:])
    arrived = exchange(sums.reshape(nplane, nx, wide), PLANE)

    other_batch = from_other_core(batch)
    kze = dot(kernel(here, sub_rows), vec_rows)
    kze = kze + from_other_core(dot(kernel(there, sub_rows), vec_rows))
    kze_sum = kze[:held]
    for k in range(1, nx):
        kze_sum = kze_sum + to_next(kze[k * held : (k + 1) * held], X, -k)
    kbz = kernel(centers, batch)
    other_kbz = kernel(centers, other_batch)

    def device_of(number, core):
        return (number % nplane * nx + number // nplane) * 2 + core

    total = jnp.sum(arrived, axis=0)
    numbers = lax.axis_index(PLANE) * nx + jnp.arange(nx, dtype=jnp.int32)
    found = owner[None, :] == device_of(numbers, my_core)[:, None]
    row_labels = jnp.sum(jnp.where(found, labels[None, :], 0), axis=1)
    mark = row_labels[:, None] == my_x * block + jnp.arange(block, dtype=jnp.int32)[None, :]
    at_label = jnp.sum(jnp.where(mark, total[:, :block] - 1.0, 0.0), axis=1, keepdims=True)
    proj = total[:, block : block + ranks] + total[:, block + ranks : block + 2 * ranks]
    ready = [total[:, :block].astype(jnp.bfloat16), *parts_of(proj, 2), at_label.astype(jnp.bfloat16)]
    ready = with_columns(jnp.concatenate(ready, axis=1), wide)
    rows = exchange(to_each(ready, PLANE), PLANE).reshape(half, wide)
    own_half = exchange(to_each(rows, X), X)
    other_half = from_other_core(own_half)

    left = jnp.concatenate([kze_sum, -eigvecs.astype(jnp.float32)], axis=0) * scales[None, :]
    left = left.reshape(held + points, nx, ranks)
    left = with_columns(jnp.concatenate([left, left], axis=2), wide - block)
    left = parts_of(left.reshape(held + points, nx * (wide - block)), 2)

    numbers = jnp.arange(half, dtype=jnp.int32)
    gradient, predictions = 0.0, 0.0
    for half_rows, core, near in ((own_half, my_core, kbz), (other_half, 1 - my_core, other_kbz)):
        chosen = owner[:, None] == device_of(numbers, core)[None, :]
        label = jnp.sum(jnp.where(chosen, labels[:, None], 0), axis=0)
        pred = jnp.concatenate([half_rows[i, :, :block] for i in range(nx)], axis=1)[:, :classes]
        predictions = predictions + dot(chosen.astype(jnp.bfloat16), pred)
        value = half_rows[:, :, block + label_at].astype(jnp.float32).sum(axis=0)
        mark = label[:, None] == jnp.arange(classes, dtype=jnp.int32)[None, :]
        resid = jnp.where(mark, value[:, None].astype(jnp.bfloat16), pred)
        proj = jnp.concatenate([half_rows[i, :, block:] for i in range(nx)], axis=1)
        back = sum(dot(piece, proj, ((1,), (1,))) for piece in left)
        near = jnp.pad(near.astype(jnp.float32), ((0, points), (0, 0)))
        gradient = gradient + sum(
            dot(resid, piece, ((0,), (1,))) for piece in parts_of(near - back, 2)
        )
    center_grad = gradient[:, :held].astype(jnp.bfloat16).T
    return (predictions.astype(jnp.bfloat16), center_grad, gradient[:, held:].T)


def solution(mesh):
    finer = Mesh(mesh.devices.reshape(mesh.shape["blk"], 8, 4, 2), ALL)
    return jax.shard_map(
        step,
        mesh=finer,
        in_specs=(
            P(ALL, None),
            P(ALL, None),
            P(),
            P(),
            P(ALL),
            P(ALL, None),
            P(),
        ),
        out_specs=(P(), P(ALL, None), P(ALL, None)),
        check_vma=False,
    )
```

```python
import jax
import jax.numpy as jnp
from jax import lax
from jax.experimental.layout import Layout, with_layout_constraint
from jax.sharding import Mesh
from jax.sharding import PartitionSpec as P

Z, Y, X, CORE = "blk", "grid_0", "grid_1", "grid_2"
ALL = (Z, Y, X, CORE)
PLANE = (Z, Y)

SOFTEN = 1.0
SPREAD = 4.0
LARGEST = 3.0e38
TILE = 128


def up_to(size, step):
    return -(-size // step) * step


def exchange(pieces, axis):
    return lax.all_to_all(pieces, axis, 0, 0, tiled=True)


def to_each(array, axis):
    return jnp.broadcast_to(array[None], (lax.axis_size(axis), *array.shape))


def from_other_core(array):
    return lax.ppermute(array, CORE, [(0, 1), (1, 0)])


def to_next(array, axis, step):
    count = lax.axis_size(axis)
    return lax.ppermute(array, axis, [(i, (i + step) % count) for i in range(count)])


def squares(rows):
    return jnp.sum(jnp.square(rows.astype(jnp.float32)), axis=1)


def kernel(left, right):
    cross = lax.dot_general(
        left, right, (((1,), (1,)), ((), ())), preferred_element_type=jnp.float32
    )
    apart = squares(left)[:, None] + squares(right)[None, :] - 2.0 * cross
    soft = jnp.minimum(jnp.maximum(apart, 0.0) + SOFTEN, LARGEST)
    return jnp.exp(soft * lax.rsqrt(soft) * (-1.0 / SPREAD)).astype(jnp.bfloat16)


def rounded(array):
    return lax.reduce_precision(array, exponent_bits=8, mantissa_bits=7)


def parts_of(array, count):
    parts = []
    for _ in range(count):
        part = rounded(array)
        parts.append(part.astype(jnp.bfloat16))
        array = array - part
    return parts


def dot(left, right, contract=((1,), (0,))):
    return lax.dot_general(left, right, (contract, ((), ())), preferred_element_type=jnp.float32)


def with_columns(array, columns):
    return jnp.pad(array, [(0, 0)] * (array.ndim - 1) + [(0, columns - array.shape[-1])])


def step(centers, weights, batch_index, labels, sub_index, eigvecs, scales):
    nx, nplane = lax.axis_size(X), lax.axis_size(PLANE)
    held, depth = centers.shape
    classes = weights.shape[1]
    points, rank = eigvecs.shape
    me = lax.axis_index(ALL)
    my_x = lax.axis_index(X)
    my_core = lax.axis_index(CORE)
    block = up_to(-(-classes // nx), TILE)
    ranks = rank // nx
    wide = up_to(block + 2 * ranks + 1, TILE)
    half = nplane * nx
    label_at = 2 * ranks

    owner = batch_index // held
    places = jnp.arange(held, dtype=jnp.int32)
    taken = jnp.any(batch_index[None, :] == (me * held + places)[:, None], axis=1)
    picks = sub_index[:, None] == places[None, :]
    chosen = jnp.concatenate([picks, taken[None, :]], axis=0).astype(jnp.bfloat16)
    picks = picks.astype(jnp.bfloat16)
    rows = dot(chosen, centers).astype(jnp.bfloat16)
    subset, mine = rows[:points], rows[points:]
    near_rows = exchange(to_each(mine.reshape(nx, -1), X), X).reshape(nx, depth)

    def side_by_side(array):
        return jnp.concatenate(jnp.split(array, points // nx, axis=0), axis=1)

    def stacked(array):
        pieces = jnp.split(array, points // nx, axis=2)
        return jnp.concatenate([piece.reshape(half, -1) for piece in pieces], axis=0)

    deep = depth * points // nx
    packed = jnp.concatenate([side_by_side(subset), near_rows, side_by_side(eigvecs)], axis=1)
    in_plane = exchange(to_each(packed, PLANE), PLANE)
    batch = in_plane[:, :, deep : deep + depth].reshape(half, depth)

    def by_x(array):
        return jnp.moveaxis(array.reshape(array.shape[0], nx, -1), 1, 0)

    high, low = parts_of(dot(picks, eigvecs, ((0,), (0,))), 2)
    wts = by_x(with_columns(weights.astype(jnp.bfloat16), nx * block))
    shares = with_columns(jnp.concatenate([wts, by_x(high), by_x(low)], axis=2), wide)

    def share_for(x):
        share = lax.dynamic_index_in_dim(shares, x % nx, 0, keepdims=False)
        return jnp.concatenate([centers, share], axis=1)

    around = [share_for(my_x)] + [to_next(share_for(my_x + k), X, k) for k in range(1, nx)]
    around = jnp.concatenate(around, axis=0)
    opposite = from_other_core(around)
    here, there = around[:, :depth], opposite[:, :depth]

    sums = dot(kernel(batch, here), around[:, depth:])
    sums = sums + dot(kernel(batch, there), opposite[:, depth:])
    later, sums = lax.optimization_barrier((in_plane, sums))
    sub_rows = stacked(later[:, :, :deep])
    vec_rows = stacked(later[:, :, deep + depth :])
    arrived = exchange(sums.reshape(nplane, nx, wide), PLANE)

    other_batch = from_other_core(batch)
    kze = dot(kernel(here, sub_rows), vec_rows)
    kze = kze + from_other_core(dot(kernel(there, sub_rows), vec_rows))
    kze_sum = kze[:held]
    for k in range(1, nx):
        kze_sum = kze_sum + to_next(kze[k * held : (k + 1) * held], X, -k)
    kbz = kernel(centers, batch)
    other_kbz = kernel(centers, other_batch)

    def device_of(number, core):
        return number * 2 + core

    total = jnp.sum(arrived, axis=0)
    numbers = lax.axis_index(PLANE) * nx + jnp.arange(nx, dtype=jnp.int32)
    found = owner[None, :] == device_of(numbers, my_core)[:, None]
    row_labels = jnp.sum(jnp.where(found, labels[None, :], 0), axis=1)
    mark = row_labels[:, None] == my_x * block + jnp.arange(block, dtype=jnp.int32)[None, :]
    at_label = jnp.sum(jnp.where(mark, total[:, :block] - 1.0, 0.0), axis=1, keepdims=True)
    proj = total[:, block : block + ranks] + total[:, block + ranks : block + 2 * ranks]
    ready = [total[:, :block].astype(jnp.bfloat16), *parts_of(proj, 2), at_label.astype(jnp.bfloat16)]
    ready = with_columns(jnp.concatenate(ready, axis=1), wide)
    rows = exchange(to_each(ready, PLANE), PLANE).reshape(half, wide)
    own_half = exchange(to_each(rows, X), X)
    other_half = from_other_core(own_half)

    left = jnp.concatenate([kze_sum, -eigvecs.astype(jnp.float32)], axis=0) * scales[None, :]
    left = left.reshape(held + points, nx, ranks)
    left = with_columns(jnp.concatenate([left, left], axis=2), wide - block)
    left = parts_of(left.reshape(held + points, nx * (wide - block)), 2)

    numbers = jnp.arange(half, dtype=jnp.int32)
    gradient, predictions = 0.0, 0.0
    for half_rows, core, near in ((own_half, my_core, kbz), (other_half, 1 - my_core, other_kbz)):
        chosen = owner[:, None] == device_of(numbers, core)[None, :]
        label = jnp.sum(jnp.where(chosen, labels[:, None], 0), axis=0)
        pred = jnp.concatenate([half_rows[i, :, :block] for i in range(nx)], axis=1)[:, :classes]
        predictions = predictions + dot(chosen.astype(jnp.bfloat16), pred)
        value = half_rows[:, :, block + label_at].astype(jnp.float32).sum(axis=0)
        mark = label[:, None] == jnp.arange(classes, dtype=jnp.int32)[None, :]
        resid = jnp.where(mark, value[:, None].astype(jnp.bfloat16), pred)
        proj = jnp.concatenate([half_rows[i, :, block:] for i in range(nx)], axis=1)
        back = sum(dot(piece, proj, ((1,), (1,))) for piece in left)
        near = jnp.pad(near.astype(jnp.float32), ((0, points), (0, 0)))
        gradient = gradient + sum(
            dot(resid, piece, ((0,), (1,))) for piece in parts_of(near - back, 2)
        )
    gradient = with_layout_constraint(gradient, Layout((0, 1)))
    center_grad = gradient[:, :held].astype(jnp.bfloat16).T
    return (predictions.astype(jnp.bfloat16), center_grad, gradient[:, held:].T)


def solution(mesh):
    finer = Mesh(mesh.devices.reshape(mesh.shape["blk"], 8, 4, 2), ALL)
    return jax.shard_map(
        step,
        mesh=finer,
        in_specs=(
            P(ALL, None),
            P(ALL, None),
            P(),
            P(),
            P(ALL),
            P(ALL, None),
            P(),
        ),
        out_specs=(P(), P(ALL, None), P(ALL, None)),
        check_vma=False,
    )
```

```python
import jax
import jax.numpy as jnp
from jax import lax
from jax.experimental import pallas as pl
from jax.experimental.pallas import tpu as pltpu
from jax.sharding import Mesh
from jax.sharding import PartitionSpec as P

Z, Y, X, CORE = "blk", "grid_0", "grid_1", "grid_2"
ALL = (Z, Y, X, CORE)
PLANE = (Z, Y)

SOFTEN = 1.0
SPREAD = 4.0
LARGEST = 3.0e38
TILE = 128


def up_to(size, step):
    return -(-size // step) * step


def exchange(pieces, axis):
    return lax.all_to_all(pieces, axis, 0, 0, tiled=True)


def to_each(array, axis):
    return jnp.broadcast_to(array[None], (lax.axis_size(axis), *array.shape))


def from_other_core(array):
    return lax.ppermute(array, CORE, [(0, 1), (1, 0)])


def to_next(array, axis, step):
    count = lax.axis_size(axis)
    return lax.ppermute(array, axis, [(i, (i + step) % count) for i in range(count)])


def squares(rows):
    return jnp.sum(jnp.square(rows.astype(jnp.float32)), axis=1)


def kernel(left, right):
    cross = lax.dot_general(
        left, right, (((1,), (1,)), ((), ())), preferred_element_type=jnp.float32
    )
    apart = squares(left)[:, None] + squares(right)[None, :] - 2.0 * cross
    soft = jnp.minimum(jnp.maximum(apart, 0.0) + SOFTEN, LARGEST)
    return jnp.exp(soft * lax.rsqrt(soft) * (-1.0 / SPREAD)).astype(jnp.bfloat16)


def rounded(array):
    return lax.reduce_precision(array, exponent_bits=8, mantissa_bits=7)


def parts_of(array, count):
    parts = []
    for _ in range(count):
        part = rounded(array)
        parts.append(part.astype(jnp.bfloat16))
        array = array - part
    return parts


def dot(left, right, contract=((1,), (0,))):
    return lax.dot_general(left, right, (contract, ((), ())), preferred_element_type=jnp.float32)


def with_columns(array, columns):
    return jnp.pad(array, [(0, 0)] * (array.ndim - 1) + [(0, columns - array.shape[-1])])


def packed_rows(batch_index, sub_index, centers, eigvecs, copies):
    held, depth = centers.shape
    points, rank = eigvecs.shape
    piece = depth // points

    def body(sub_ref, batch_ref, centers_ref, eigvecs_ref, out_ref):
        start = lax.axis_index(ALL) * held
        within = batch_ref[...] - start
        inside = jnp.logical_and(within >= 0, within < held)
        row = jnp.sum(jnp.where(inside, within, 0).astype(jnp.float32)).astype(jnp.int32)
        lines = lax.broadcasted_iota(jnp.int32, (2 * points, held), 0)
        target = jnp.full((2 * points, held), row, jnp.int32)
        for i in range(points):
            target = jnp.where(lines == i, sub_ref[i], target)
        lanes = lax.broadcasted_iota(jnp.int32, (2 * points, held), 1)
        picks = jnp.where(lanes == target, 1.0, 0.0).astype(jnp.bfloat16)
        rows = dot(picks, centers_ref[...])
        mine = rows[points:]
        line = lax.broadcasted_iota(jnp.int32, (points, piece), 0)
        block = mine[:, :piece]
        for i in range(1, points):
            block = jnp.where(line == i, mine[:, i * piece : (i + 1) * piece], block)
        vecs = eigvecs_ref[...].astype(jnp.float32)
        packed = jnp.concatenate([rows[:points], vecs, block], axis=1).astype(jnp.bfloat16)
        out_ref[...] = jnp.broadcast_to(packed[None], out_ref.shape)

    return pl.pallas_call(
        body,
        out_shape=jax.ShapeDtypeStruct((copies, points, depth + rank + piece), jnp.bfloat16),
        in_specs=[
            pl.BlockSpec(memory_space=pltpu.SMEM),
            pl.BlockSpec(memory_space=pltpu.VMEM),
            pl.BlockSpec(memory_space=pltpu.VMEM),
            pl.BlockSpec(memory_space=pltpu.VMEM),
        ],
        out_specs=pl.BlockSpec(memory_space=pltpu.VMEM),
        name="packed_rows",
    )(sub_index, batch_index.reshape(-1, min(TILE, batch_index.shape[0])), centers, eigvecs)


def step(centers, weights, batch_index, labels, sub_index, eigvecs, scales):
    nx, nplane = lax.axis_size(X), lax.axis_size(PLANE)
    held, depth = centers.shape
    classes = weights.shape[1]
    points, rank = eigvecs.shape
    my_x = lax.axis_index(X)
    my_core = lax.axis_index(CORE)
    block = up_to(-(-classes // nx), TILE)
    ranks = rank // nx
    wide = up_to(block + 2 * ranks + 1, TILE)
    half = nplane * nx
    label_at = 2 * ranks

    owner = batch_index // held
    packed = packed_rows(batch_index, sub_index, centers, eigvecs, nplane)
    in_plane = exchange(packed, PLANE)
    sub_rows = in_plane[:, :, :depth].reshape(nplane * points, depth)
    vec_rows = in_plane[:, :, depth : depth + rank].reshape(nplane * points, rank)
    column = in_plane[:, :, depth + rank :].reshape(nplane, depth)
    batch = exchange(to_each(column, X), X).reshape(half, depth)

    def by_x(array):
        return jnp.moveaxis(array.reshape(array.shape[0], nx, -1), 1, 0)

    picks = sub_index[:, None] == jnp.arange(held, dtype=jnp.int32)[None, :]
    picks = picks.astype(jnp.bfloat16)
    high, low = parts_of(dot(picks, eigvecs, ((0,), (0,))), 2)
    wts = by_x(with_columns(weights.astype(jnp.bfloat16), nx * block))
    shares = with_columns(jnp.concatenate([wts, by_x(high), by_x(low)], axis=2), wide)

    def share_for(x):
        share = lax.dynamic_index_in_dim(shares, x % nx, 0, keepdims=False)
        return jnp.concatenate([centers, share], axis=1)

    around = [share_for(my_x)] + [to_next(share_for(my_x + k), X, k) for k in range(1, nx)]
    around = jnp.concatenate(around, axis=0)
    opposite = from_other_core(around)
    here, there = around[:, :depth], opposite[:, :depth]

    sums = dot(kernel(batch, here), around[:, depth:])
    sums = sums + dot(kernel(batch, there), opposite[:, depth:])
    arrived = exchange(sums.reshape(nplane, nx, wide), PLANE)

    other_batch = from_other_core(batch)
    kze = dot(kernel(here, sub_rows), vec_rows)
    kze = kze + from_other_core(dot(kernel(there, sub_rows), vec_rows))
    kze_sum = kze[:held]
    for k in range(1, nx):
        kze_sum = kze_sum + to_next(kze[k * held : (k + 1) * held], X, -k)
    kbz = kernel(centers, batch)
    other_kbz = kernel(centers, other_batch)

    def device_of(number, core):
        return (number % nplane * nx + number // nplane) * 2 + core

    total = jnp.sum(arrived, axis=0)
    numbers = lax.axis_index(PLANE) * nx + jnp.arange(nx, dtype=jnp.int32)
    found = owner[None, :] == device_of(numbers, my_core)[:, None]
    row_labels = jnp.sum(jnp.where(found, labels[None, :], 0), axis=1)
    mark = row_labels[:, None] == my_x * block + jnp.arange(block, dtype=jnp.int32)[None, :]
    at_label = jnp.sum(jnp.where(mark, total[:, :block] - 1.0, 0.0), axis=1, keepdims=True)
    proj = total[:, block : block + ranks] + total[:, block + ranks : block + 2 * ranks]
    ready = [total[:, :block].astype(jnp.bfloat16), *parts_of(proj, 2), at_label.astype(jnp.bfloat16)]
    ready = with_columns(jnp.concatenate(ready, axis=1), wide)
    rows = exchange(to_each(ready, PLANE), PLANE).reshape(half, wide)
    own_half = exchange(to_each(rows, X), X)
    other_half = from_other_core(own_half)

    left = jnp.concatenate([kze_sum, -eigvecs.astype(jnp.float32)], axis=0) * scales[None, :]
    left = left.reshape(held + points, nx, ranks)
    left = with_columns(jnp.concatenate([left, left], axis=2), wide - block)
    left = parts_of(left.reshape(held + points, nx * (wide - block)), 2)

    numbers = jnp.arange(half, dtype=jnp.int32)
    gradient, predictions = 0.0, 0.0
    for half_rows, core, near in ((own_half, my_core, kbz), (other_half, 1 - my_core, other_kbz)):
        chosen = owner[:, None] == device_of(numbers, core)[None, :]
        label = jnp.sum(jnp.where(chosen, labels[:, None], 0), axis=0)
        pred = jnp.concatenate([half_rows[i, :, :block] for i in range(nx)], axis=1)[:, :classes]
        predictions = predictions + dot(pred, chosen.astype(jnp.bfloat16), ((0,), (1,)))
        value = half_rows[:, :, block + label_at].astype(jnp.float32).sum(axis=0)
        mark = label[:, None] == jnp.arange(classes, dtype=jnp.int32)[None, :]
        resid = jnp.where(mark, value[:, None].astype(jnp.bfloat16), pred)
        proj = jnp.concatenate([half_rows[i, :, block:] for i in range(nx)], axis=1)
        back = sum(dot(piece, proj, ((1,), (1,))) for piece in left)
        near = jnp.pad(near.astype(jnp.float32), ((0, points), (0, 0)))
        gradient = gradient + sum(
            dot(resid, piece, ((0,), (1,))) for piece in parts_of(near - back, 2)
        )
    center_grad = gradient[:, :held].astype(jnp.bfloat16).T
    return (predictions.astype(jnp.bfloat16).T, center_grad, gradient[:, held:].T)


def solution(mesh):
    finer = Mesh(mesh.devices.reshape(mesh.shape["blk"], 8, 4, 2), ALL)
    return jax.shard_map(
        step,
        mesh=finer,
        in_specs=(
            P(ALL, None),
            P(ALL, None),
            P(),
            P(),
            P(ALL),
            P(ALL, None),
            P(),
        ),
        out_specs=(P(), P(ALL, None), P(ALL, None)),
        check_vma=False,
    )
```

```python
import jax
import jax.numpy as jnp
from jax import lax
from jax.experimental import pallas as pl
from jax.experimental.pallas import tpu as pltpu
from jax.sharding import Mesh
from jax.sharding import PartitionSpec as P

Z, Y, X, CORE = "blk", "grid_0", "grid_1", "grid_2"
ALL = (Z, Y, X, CORE)
PLANE = (Z, Y)

SOFTEN = 1.0
SPREAD = 4.0
LARGEST = 3.0e38
TILE = 128


def up_to(size, step):
    return -(-size // step) * step


def exchange(pieces, axis):
    return lax.all_to_all(pieces, axis, 0, 0, tiled=True)


def to_each(array, axis):
    return jnp.broadcast_to(array[None], (lax.axis_size(axis), *array.shape))


def from_other_core(array):
    return lax.ppermute(array, CORE, [(0, 1), (1, 0)])


def to_next(array, axis, step):
    count = lax.axis_size(axis)
    return lax.ppermute(array, axis, [(i, (i + step) % count) for i in range(count)])


def squares(rows):
    return jnp.sum(jnp.square(rows.astype(jnp.float32)), axis=1)


def kernel(left, right):
    cross = lax.dot_general(
        left, right, (((1,), (1,)), ((), ())), preferred_element_type=jnp.float32
    )
    apart = squares(left)[:, None] + squares(right)[None, :] - 2.0 * cross
    soft = jnp.minimum(jnp.maximum(apart, 0.0) + SOFTEN, LARGEST)
    return jnp.exp(soft * lax.rsqrt(soft) * (-1.0 / SPREAD)).astype(jnp.bfloat16)


def rounded(array):
    return lax.reduce_precision(array, exponent_bits=8, mantissa_bits=7)


def parts_of(array, count):
    parts = []
    for _ in range(count):
        part = rounded(array)
        parts.append(part.astype(jnp.bfloat16))
        array = array - part
    return parts


def dot(left, right, contract=((1,), (0,))):
    return lax.dot_general(left, right, (contract, ((), ())), preferred_element_type=jnp.float32)


def dot_pieces(pieces, right, contract):
    count = pieces[0].shape[0]
    both = dot(jnp.concatenate(pieces, axis=0), right, contract)
    return both[:count] + both[count:]


def with_columns(array, columns):
    return jnp.pad(array, [(0, 0)] * (array.ndim - 1) + [(0, columns - array.shape[-1])])


def packed_rows(batch_index, sub_index, centers, eigvecs, copies):
    held, depth = centers.shape
    points, rank = eigvecs.shape
    piece = depth // points

    def body(sub_ref, batch_ref, centers_ref, eigvecs_ref, out_ref):
        start = lax.axis_index(ALL) * held
        within = batch_ref[...] - start
        inside = jnp.logical_and(within >= 0, within < held)
        row = jnp.sum(jnp.where(inside, within, 0).astype(jnp.float32)).astype(jnp.int32)
        lines = lax.broadcasted_iota(jnp.int32, (2 * points, held), 0)
        target = jnp.full((2 * points, held), row, jnp.int32)
        for i in range(points):
            target = jnp.where(lines == i, sub_ref[i], target)
        lanes = lax.broadcasted_iota(jnp.int32, (2 * points, held), 1)
        picks = jnp.where(lanes == target, 1.0, 0.0).astype(jnp.bfloat16)
        rows = dot(picks, centers_ref[...])
        mine = rows[points:]
        line = lax.broadcasted_iota(jnp.int32, (points, piece), 0)
        block = mine[:, :piece]
        for i in range(1, points):
            block = jnp.where(line == i, mine[:, i * piece : (i + 1) * piece], block)
        vecs = eigvecs_ref[...].astype(jnp.float32)
        packed = jnp.concatenate([rows[:points], vecs, block], axis=1).astype(jnp.bfloat16)
        out_ref[...] = jnp.broadcast_to(packed[None], out_ref.shape)

    return pl.pallas_call(
        body,
        out_shape=jax.ShapeDtypeStruct((copies, points, depth + rank + piece), jnp.bfloat16),
        in_specs=[
            pl.BlockSpec(memory_space=pltpu.SMEM),
            pl.BlockSpec(memory_space=pltpu.VMEM),
            pl.BlockSpec(memory_space=pltpu.VMEM),
            pl.BlockSpec(memory_space=pltpu.VMEM),
        ],
        out_specs=pl.BlockSpec(memory_space=pltpu.VMEM),
        name="packed_rows",
    )(sub_index, batch_index.reshape(-1, min(TILE, batch_index.shape[0])), centers, eigvecs)


def step(centers, weights, batch_index, labels, sub_index, eigvecs, scales):
    nx, nplane = lax.axis_size(X), lax.axis_size(PLANE)
    held, depth = centers.shape
    classes = weights.shape[1]
    points, rank = eigvecs.shape
    my_x = lax.axis_index(X)
    my_core = lax.axis_index(CORE)
    block = up_to(-(-classes // nx), TILE)
    ranks = rank // nx
    wide = up_to(block + 2 * ranks + 1, TILE)
    half = nplane * nx
    label_at = 2 * ranks

    owner = batch_index // held
    packed = packed_rows(batch_index, sub_index, centers, eigvecs, nplane)
    in_plane = exchange(packed, PLANE)
    sub_rows = in_plane[:, :, :depth].reshape(nplane * points, depth)
    vec_rows = in_plane[:, :, depth : depth + rank].reshape(nplane * points, rank)
    column = in_plane[:, :, depth + rank :].reshape(nplane, depth)
    batch = exchange(to_each(column, X), X).reshape(half, depth)

    def by_x(array):
        return jnp.moveaxis(array.reshape(array.shape[0], nx, -1), 1, 0)

    picks = sub_index[:, None] == jnp.arange(held, dtype=jnp.int32)[None, :]
    picks = picks.astype(jnp.bfloat16)
    high, low = parts_of(dot(picks, eigvecs, ((0,), (0,))), 2)
    wts = by_x(with_columns(weights.astype(jnp.bfloat16), nx * block))
    shares = with_columns(jnp.concatenate([wts, by_x(high), by_x(low)], axis=2), wide)

    def share_for(x):
        share = lax.dynamic_index_in_dim(shares, x % nx, 0, keepdims=False)
        return jnp.concatenate([centers, share], axis=1)

    around = [share_for(my_x)] + [to_next(share_for(my_x + k), X, k) for k in range(1, nx)]
    around = jnp.concatenate(around, axis=0)
    opposite = from_other_core(around)
    here, there = around[:, :depth], opposite[:, :depth]

    sums = dot(kernel(batch, here), around[:, depth:])
    sums = sums + dot(kernel(batch, there), opposite[:, depth:])
    arrived = exchange(sums.reshape(nplane, nx, wide), PLANE)

    other_batch = from_other_core(batch)
    kze = dot(kernel(here, sub_rows), vec_rows)
    kze = kze + from_other_core(dot(kernel(there, sub_rows), vec_rows))
    kze_sum = kze[:held]
    for k in range(1, nx):
        kze_sum = kze_sum + to_next(kze[k * held : (k + 1) * held], X, -k)
    kbz = kernel(centers, batch)
    other_kbz = kernel(centers, other_batch)

    def device_of(number, core):
        return (number % nplane * nx + number // nplane) * 2 + core

    total = jnp.sum(arrived, axis=0)
    numbers = lax.axis_index(PLANE) * nx + jnp.arange(nx, dtype=jnp.int32)
    found = owner[None, :] == device_of(numbers, my_core)[:, None]
    row_labels = jnp.sum(jnp.where(found, labels[None, :], 0), axis=1)
    mark = row_labels[:, None] == my_x * block + jnp.arange(block, dtype=jnp.int32)[None, :]
    at_label = jnp.sum(jnp.where(mark, total[:, :block] - 1.0, 0.0), axis=1, keepdims=True)
    proj = total[:, block : block + ranks] + total[:, block + ranks : block + 2 * ranks]
    ready = [total[:, :block].astype(jnp.bfloat16), *parts_of(proj, 2), at_label.astype(jnp.bfloat16)]
    ready = with_columns(jnp.concatenate(ready, axis=1), wide)
    rows = exchange(to_each(ready, PLANE), PLANE).reshape(half, wide)
    own_half = exchange(to_each(rows, X), X)
    other_half = from_other_core(own_half)

    left = jnp.concatenate([kze_sum, -eigvecs.astype(jnp.float32)], axis=0) * scales[None, :]
    left = left.reshape(held + points, nx, ranks)
    left = with_columns(jnp.concatenate([left, left], axis=2), wide - block)
    left = parts_of(left.reshape(held + points, nx * (wide - block)), 2)

    numbers = jnp.arange(half, dtype=jnp.int32)
    gradient, predictions = 0.0, 0.0
    for half_rows, core, near in ((own_half, my_core, kbz), (other_half, 1 - my_core, other_kbz)):
        chosen = owner[:, None] == device_of(numbers, core)[None, :]
        label = jnp.sum(jnp.where(chosen, labels[:, None], 0), axis=0)
        pred = jnp.concatenate([half_rows[i, :, :block] for i in range(nx)], axis=1)[:, :classes]
        placed = dot(pred, chosen.astype(jnp.bfloat16), ((0,), (1,)))
        predictions = (predictions + placed).astype(jnp.bfloat16)
        value = half_rows[:, :, block + label_at].astype(jnp.float32).sum(axis=0)
        mark = label[:, None] == jnp.arange(classes, dtype=jnp.int32)[None, :]
        resid = jnp.where(mark, value[:, None].astype(jnp.bfloat16), pred)
        proj = jnp.concatenate([half_rows[i, :, block:] for i in range(nx)], axis=1)
        back = dot_pieces(left, proj, ((1,), (1,)))
        near = jnp.pad(near.astype(jnp.float32), ((0, points), (0, 0)))
        gradient = gradient + dot_pieces(parts_of(near - back, 2), resid, ((1,), (0,)))
    center_grad = gradient[:held].astype(jnp.bfloat16)
    return (predictions.T, center_grad, gradient[held:])


def solution(mesh):
    finer = Mesh(mesh.devices.reshape(mesh.shape["blk"], 8, 4, 2), ALL)
    return jax.shard_map(
        step,
        mesh=finer,
        in_specs=(
            P(ALL, None),
            P(ALL, None),
            P(),
            P(),
            P(ALL),
            P(ALL, None),
            P(),
        ),
        out_specs=(P(), P(ALL, None), P(ALL, None)),
        check_vma=False,
    )
```

```python
import jax
import jax.numpy as jnp
from jax import lax
from jax.experimental import pallas as pl
from jax.experimental.pallas import tpu as pltpu
from jax.sharding import Mesh
from jax.sharding import PartitionSpec as P

Z, Y, X, CORE = "blk", "grid_0", "grid_1", "grid_2"
ALL = (Z, Y, X, CORE)
PLANE = (Z, Y)

SOFTEN = 1.0
SPREAD = 4.0
LARGEST = 3.0e38
TILE = 128


def up_to(size, step):
    return -(-size // step) * step


def exchange(pieces, axis):
    return lax.all_to_all(pieces, axis, 0, 0, tiled=True)


def to_each(array, axis):
    return jnp.broadcast_to(array[None], (lax.axis_size(axis), *array.shape))


def from_other_core(array):
    return lax.ppermute(array, CORE, [(0, 1), (1, 0)])


def to_next(array, axis, step):
    count = lax.axis_size(axis)
    return lax.ppermute(array, axis, [(i, (i + step) % count) for i in range(count)])


def squares(rows):
    return jnp.sum(jnp.square(rows.astype(jnp.float32)), axis=1)


def kernel(left, right):
    cross = lax.dot_general(
        left, right, (((1,), (1,)), ((), ())), preferred_element_type=jnp.float32
    )
    apart = squares(left)[:, None] + squares(right)[None, :] - 2.0 * cross
    soft = jnp.minimum(jnp.maximum(apart, 0.0) + SOFTEN, LARGEST)
    return jnp.exp(soft * lax.rsqrt(soft) * (-1.0 / SPREAD)).astype(jnp.bfloat16)


def rounded(array):
    return lax.reduce_precision(array, exponent_bits=8, mantissa_bits=7)


def parts_of(array, count):
    parts = []
    for _ in range(count):
        part = rounded(array)
        parts.append(part.astype(jnp.bfloat16))
        array = array - part
    return parts


def dot(left, right, contract=((1,), (0,))):
    return lax.dot_general(left, right, (contract, ((), ())), preferred_element_type=jnp.float32)


def with_columns(array, columns):
    return jnp.pad(array, [(0, 0)] * (array.ndim - 1) + [(0, columns - array.shape[-1])])


def packed_rows(batch_index, sub_index, centers, eigvecs, copies):
    held, depth = centers.shape
    points, rank = eigvecs.shape
    piece = depth // points

    def body(sub_ref, batch_ref, centers_ref, eigvecs_ref, out_ref):
        start = lax.axis_index(ALL) * held
        within = batch_ref[...] - start
        inside = jnp.logical_and(within >= 0, within < held)
        hits = jnp.where(inside, within, 0).astype(jnp.float32)
        row = jnp.sum(jnp.sum(hits, axis=0, keepdims=True), axis=1, keepdims=True)
        lines = lax.broadcasted_iota(jnp.int32, (2 * points, held), 0)
        target = jnp.broadcast_to(row.astype(jnp.int32), (2 * points, held))
        for i in range(points):
            target = jnp.where(lines == i, sub_ref[i], target)
        lanes = lax.broadcasted_iota(jnp.int32, (2 * points, held), 1)
        picks = jnp.where(lanes == target, 1.0, 0.0).astype(jnp.bfloat16)
        rows = dot(picks, centers_ref[...])
        mine = rows[points:]
        line = lax.broadcasted_iota(jnp.int32, (points, piece), 0)
        block = mine[:, :piece]
        for i in range(1, points):
            block = jnp.where(line == i, mine[:, i * piece : (i + 1) * piece], block)
        vecs = eigvecs_ref[...].astype(jnp.float32)
        packed = jnp.concatenate([rows[:points], vecs, block], axis=1).astype(jnp.bfloat16)
        out_ref[...] = jnp.broadcast_to(packed[None], out_ref.shape)

    return pl.pallas_call(
        body,
        out_shape=jax.ShapeDtypeStruct((copies, points, depth + rank + piece), jnp.bfloat16),
        in_specs=[
            pl.BlockSpec(memory_space=pltpu.SMEM),
            pl.BlockSpec(memory_space=pltpu.VMEM),
            pl.BlockSpec(memory_space=pltpu.VMEM),
            pl.BlockSpec(memory_space=pltpu.VMEM),
        ],
        out_specs=pl.BlockSpec(memory_space=pltpu.VMEM),
        name="packed_rows",
    )(sub_index, batch_index.reshape(-1, min(TILE, batch_index.shape[0])), centers, eigvecs)


def step(centers, weights, batch_index, labels, sub_index, eigvecs, scales):
    nx, nplane = lax.axis_size(X), lax.axis_size(PLANE)
    held, depth = centers.shape
    classes = weights.shape[1]
    points, rank = eigvecs.shape
    my_x = lax.axis_index(X)
    my_core = lax.axis_index(CORE)
    block = up_to(-(-classes // nx), TILE)
    ranks = rank // nx
    wide = up_to(block + 2 * ranks + 1, TILE)
    half = nplane * nx
    label_at = 2 * ranks

    owner = batch_index // held
    packed = packed_rows(batch_index, sub_index, centers, eigvecs, nplane)
    in_plane = exchange(packed, PLANE)
    sub_rows = in_plane[:, :, :depth].reshape(nplane * points, depth)
    vec_rows = in_plane[:, :, depth : depth + rank].reshape(nplane * points, rank)
    column = in_plane[:, :, depth + rank :].reshape(nplane, depth)
    batch = exchange(to_each(column, X), X).reshape(half, depth)

    def by_x(array):
        return jnp.moveaxis(array.reshape(array.shape[0], nx, -1), 1, 0)

    picks = sub_index[:, None] == jnp.arange(held, dtype=jnp.int32)[None, :]
    picks = picks.astype(jnp.bfloat16)
    high, low = parts_of(dot(picks, eigvecs, ((0,), (0,))), 2)
    wts = by_x(with_columns(weights.astype(jnp.bfloat16), nx * block))
    shares = with_columns(jnp.concatenate([wts, by_x(high), by_x(low)], axis=2), wide)

    def share_for(x):
        share = lax.dynamic_index_in_dim(shares, x % nx, 0, keepdims=False)
        return jnp.concatenate([centers, share], axis=1)

    around = [share_for(my_x)] + [to_next(share_for(my_x + k), X, k) for k in range(1, nx)]
    around = jnp.concatenate(around, axis=0)
    opposite = from_other_core(around)
    here, there = around[:, :depth], opposite[:, :depth]

    sums = dot(kernel(batch, here), around[:, depth:])
    sums = sums + dot(kernel(batch, there), opposite[:, depth:])
    arrived = exchange(sums.reshape(nplane, nx, wide), PLANE)

    other_batch = from_other_core(batch)
    kze = dot(kernel(here, sub_rows), vec_rows)
    kze = kze + from_other_core(dot(kernel(there, sub_rows), vec_rows))
    kze_sum = kze[:held]
    for k in range(1, nx):
        kze_sum = kze_sum + to_next(kze[k * held : (k + 1) * held], X, -k)
    kbz = kernel(centers, batch)
    other_kbz = kernel(centers, other_batch)

    def device_of(number, core):
        return (number % nplane * nx + number // nplane) * 2 + core

    total = jnp.sum(arrived, axis=0)
    numbers = lax.axis_index(PLANE) * nx + jnp.arange(nx, dtype=jnp.int32)
    found = owner[None, :] == device_of(numbers, my_core)[:, None]
    row_labels = jnp.sum(jnp.where(found, labels[None, :], 0), axis=1)
    mark = row_labels[:, None] == my_x * block + jnp.arange(block, dtype=jnp.int32)[None, :]
    at_label = jnp.sum(jnp.where(mark, total[:, :block] - 1.0, 0.0), axis=1, keepdims=True)
    proj = total[:, block : block + ranks] + total[:, block + ranks : block + 2 * ranks]
    ready = [total[:, :block].astype(jnp.bfloat16), *parts_of(proj, 2), at_label.astype(jnp.bfloat16)]
    ready = with_columns(jnp.concatenate(ready, axis=1), wide)
    rows = exchange(to_each(ready, PLANE), PLANE).reshape(half, wide)
    own_half = exchange(to_each(rows, X), X)
    other_half = from_other_core(own_half)

    left = jnp.concatenate([kze_sum, -eigvecs.astype(jnp.float32)], axis=0) * scales[None, :]
    left = left.reshape(held + points, nx, ranks)
    left = with_columns(jnp.concatenate([left, left], axis=2), wide - block)
    left = parts_of(left.reshape(held + points, nx * (wide - block)), 2)

    numbers = jnp.arange(half, dtype=jnp.int32)
    gradient, predictions = 0.0, 0.0
    for half_rows, core, near in ((own_half, my_core, kbz), (other_half, 1 - my_core, other_kbz)):
        chosen = owner[:, None] == device_of(numbers, core)[None, :]
        label = jnp.sum(jnp.where(chosen, labels[:, None], 0), axis=0)
        pred = jnp.concatenate([half_rows[i, :, :block] for i in range(nx)], axis=1)[:, :classes]
        predictions = predictions + dot(pred, chosen.astype(jnp.bfloat16), ((0,), (1,)))
        value = half_rows[:, :, block + label_at].astype(jnp.float32).sum(axis=0)
        mark = label[:, None] == jnp.arange(classes, dtype=jnp.int32)[None, :]
        resid = jnp.where(mark, value[:, None].astype(jnp.bfloat16), pred)
        proj = jnp.concatenate([half_rows[i, :, block:] for i in range(nx)], axis=1)
        back = sum(dot(piece, proj, ((1,), (1,))) for piece in left)
        near = jnp.pad(near.astype(jnp.float32), ((0, points), (0, 0)))
        gradient = gradient + sum(
            dot(resid, piece, ((0,), (1,))) for piece in parts_of(near - back, 2)
        )
    center_grad = gradient[:, :held].astype(jnp.bfloat16).T
    return (predictions.astype(jnp.bfloat16).T, center_grad, gradient[:, held:].T)


def solution(mesh):
    finer = Mesh(mesh.devices.reshape(mesh.shape["blk"], 8, 4, 2), ALL)
    return jax.shard_map(
        step,
        mesh=finer,
        in_specs=(
            P(ALL, None),
            P(ALL, None),
            P(),
            P(),
            P(ALL),
            P(ALL, None),
            P(),
        ),
        out_specs=(P(), P(ALL, None), P(ALL, None)),
        check_vma=False,
    )
```
